128 devices in a mesh: gz: 128 (over y, z, x, core).
Axes of the slice: x: 4, y: 4, z: 4, core: 2. Of those that a mesh axis runs over, the one named last changes fastest.
Arguments:
- scores: int32 [512, 512, 512], P('gz'), may hold values from 0 to 134217727, as said below
Outputs:
- status: int32 [512, 512, 512], P('gz')
- counts: int32 [3], replicated
The draws below stay inside these ranges and needn't reach their ends.
Inputs may be any that keep to these rules, and one draw needn't show every extreme that they name: `scores`: all values distinct: a permutation of 0 to 134217727.
All inputs are finite; a program needn't handle non-finite values.
Results may differ from the reference program's by a relative error of at most 0.000001.
Values may be sent and summed in bfloat16 or wider, within the bound.
No kernel may reach another device: no remote copies, remote signals or barrier semaphores. Data moves between devices by JAX's collectives and lax.ppermute only.
A program may use at most 64 MiB of HBM per device.

```python
import jax
import jax.numpy as jnp

NX = 512
NY = 512
ROUNDS = 3
NZ = 512


def draw_scores(key, part):
    return jax.random.permutation(key, NX * NY * NZ).astype(jnp.int32).reshape(NZ, NX, NY)


def setup_inputs(seed: int = 0) -> dict:
    splits = jax.random.split(jax.random.key(seed), 2)
    return {
        "scores": draw_scores(jax.random.fold_in(splits[1], 71), 0),
    }


ceiling = 1 << 30


def lateral_max(field):
    padded = jnp.pad(field, ((0, 0), (1, 1), (1, 1)))
    rows_max = jnp.maximum(jnp.maximum(padded[:, :-2, :], padded[:, 1:-1, :]), padded[:, 2:, :])
    return jnp.maximum(jnp.maximum(rows_max[:, :, :-2], rows_max[:, :, 1:-1]), rows_max[:, :, 2:])


def box_maximum(extended):
    depth_max = jnp.maximum(jnp.maximum(extended[:-2], extended[1:-1]), extended[2:])
    return lateral_max(depth_max)


def reference(scores):
    status = jnp.zeros(scores.shape, jnp.int32)
    totals = []
    for round_index in range(ROUNDS):
        labels = jnp.where(status == 0, 4 * scores + 4, jnp.where(status == 1, ceiling, 0)).astype(jnp.int32)
        near_max = box_maximum(jnp.pad(labels, ((1, 1), (0, 0), (0, 0))))
        far_max = box_maximum(jnp.pad(near_max, ((1, 1), (0, 0), (0, 0))))
        undecided = status == 0
        status = jnp.where(undecided & (far_max >= ceiling), 2,
                           jnp.where(undecided & (far_max == labels), 1, status)).astype(jnp.int32)
        totals.append(jnp.sum((status == 0).astype(jnp.int32)).astype(jnp.int32))
    return status, jnp.stack(totals).astype(jnp.int32)
```

```python
import functools

import jax
import jax.numpy as jnp
from jax import lax
from jax.experimental import pallas as pl
from jax.experimental.pallas import tpu as pltpu
from jax.sharding import Mesh
from jax.sharding import PartitionSpec as P

GZ = ("gz_0", "gz_1", "gz_2", "gz_3")
LANES = 128
SUB = 8
VMEM = pltpu.VMEM
I32 = jnp.int32

CUTS = (384,)


def shift_lanes(tiles, by, beyond):
    lane = lax.broadcasted_iota(I32, tiles[0].shape, 1)
    turned = [pltpu.roll(t, by % LANES, 1) for t in tiles]
    out = []
    for c in range(len(tiles)):
        if by > 0:
            other = turned[c - 1] if c > 0 else beyond
            out.append(jnp.where(lane < by, other, turned[c]))
        else:
            other = turned[c + 1] if c + 1 < len(tiles) else beyond
            out.append(jnp.where(lane >= LANES + by, other, turned[c]))
    return out


def lane_window(tiles, op, fill):
    two = [op(a, b) for a, b in zip(tiles, shift_lanes(tiles, 1, fill))]
    lane = lax.broadcasted_iota(I32, tiles[0].shape, 1)
    past = jnp.where(lane == LANES - 2, pltpu.roll(tiles[-1], LANES - 1, 1), fill)
    four = [op(a, b) for a, b in zip(two, shift_lanes(two, -2, past))]
    return [op(a, b) for a, b in zip(four, shift_lanes(tiles, 2, fill))]


def row_window(ref, index, row, op):
    out = ref[index, pl.ds(row - 2, SUB), :]
    for k in (-1, 0, 1, 2):
        out = op(out, ref[index, pl.ds(row + k, SUB), :])
    return out


class Rows:
    def __init__(self, starts, refs):
        self.starts, self.refs = starts, refs

    def split(self, lo, hi):
        edges = sorted({lo, hi, *[s for s in self.starts if lo < s < hi]})
        return list(zip(edges, edges[1:]))

    def at(self, row):
        k = max(i for i, s in enumerate(self.starts) if s <= row)
        return self.refs[k], self.starts[k]


def for_rows(lo, hi, step, sources, body, carry=None):
    edges = sorted({lo, hi, *[e for s in sources for e in s.starts if lo < e < hi]})
    for a, b in zip(edges, edges[1:]):
        def one(i, c, a=a):
            r = a + i * step

            def pick(rows):
                ref, start = rows.at(a)
                return ref, pl.multiple_of(r - start, SUB)

            return body(pl.multiple_of(r, SUB), pick, c)

        carry = lax.fori_loop(0, (b - a) // step, one, 0 if carry is None else carry)
    return carry


def tile(c):
    return pl.ds(c * LANES, LANES)


def depth_maxima(p):
    mid = jnp.maximum(p[3], p[4])
    low = jnp.maximum(p[2], mid)
    all4 = jnp.maximum(low, p[5])
    return (
        jnp.maximum(low, jnp.maximum(p[0], p[1])),
        jnp.maximum(all4, p[1]),
        jnp.maximum(all4, p[6]),
        jnp.maximum(jnp.maximum(mid, p[5]), jnp.maximum(p[6], p[7])),
    )


def load_planes(pick, far, near, own, mate, rows, c, void):
    f, fr = pick(far)
    n, nr = pick(near)
    o, orow = pick(own)
    m, mr = pick(mate)
    get = lambda ref, k, r: ref[k, pl.ds(r + rows, SUB), tile(c)]
    return [
        get(f, 1, fr) | void,
        get(f, 0, fr) | void,
        get(n, 0, nr),
        get(n, 1, nr),
        get(o, 1, orow),
        get(o, 0, orow),
        get(m, 0, mr),
        get(m, 1, mr),
    ]


def cut_kernel(where, scores, *rest, parts):
    outs, sems = rest[: len(parts)], rest[len(parts)]
    odd = where[0]
    copies = []
    for out, (kind, lo, hi) in zip(outs, parts):
        for k in range(2):
            j = k if kind == "near" else 3 - k
            plane = j + odd * (3 - 2 * j)
            copies.append(
                pltpu.make_async_copy(
                    scores.at[plane, pl.ds(lo, hi - lo), :], out.at[k], sems.at[len(copies)]
                )
            )
    for c in copies:
        c.start()
    for c in copies:
        c.wait()


def cut(where, scores, parts):
    width = scores.shape[2]
    return pl.pallas_call(
        functools.partial(cut_kernel, parts=parts),
        in_specs=[pl.BlockSpec(memory_space=pltpu.SMEM), pl.BlockSpec(memory_space=pl.ANY)],
        out_specs=[pl.BlockSpec(memory_space=VMEM) for _ in parts],
        out_shape=[jax.ShapeDtypeStruct((2, hi - lo, width), I32) for _, lo, hi in parts],
        scratch_shapes=[pltpu.SemaphoreType.DMA((2 * len(parts),))],
    )(where, scores)


def roots_kernel(where, *args, spec):
    lo, hi, height, tiles, starts, n_far = spec
    args = list(args)
    take = lambda n: [args.pop(0) for _ in range(n)]
    far, near = Rows(starts[:n_far], take(n_far)), Rows(starts, take(len(starts)))
    own, mate = Rows((0,), take(1)), Rows((0,), take(1))
    bits_out, far_out, mate_out, count_out, work = args
    void = where[1]
    base = lo - 2 * SUB

    first, last = max(lo - SUB, 0), min(hi + SUB, height)
    empty = jnp.full((SUB, LANES), -1, I32)
    for k in range(4 * tiles):
        if lo == 0:
            work[k, pl.ds(SUB, SUB), :] = empty
        if hi == height:
            work[k, pl.ds(height - base, SUB), :] = empty

    def spread(r, pick, carry):
        per_tile = [
            depth_maxima(load_planes(pick, far, near, own, mate, 0, c, void)) for c in range(tiles)
        ]
        for q in range(4):
            wide = lane_window([t[q] for t in per_tile], jnp.maximum, -1)
            for c in range(tiles):
                work[q * tiles + c, pl.ds(r - base, SUB), :] = wide[c]
        return carry

    for_rows(first, last, SUB, (far, near), spread)

    def decide(r, pick, carry):
        near_ref, nr = pick(near)
        own_ref, orow = pick(own)
        for c in range(tiles):
            to_far, to_mate = [], []
            for half in range(2):
                off = half * SUB
                bits = jnp.zeros((SUB, LANES), I32)
                ahead = jnp.zeros((SUB, LANES), I32)
                behind = jnp.zeros((SUB, LANES), I32)
                for q in range(4):
                    ref, row = (near_ref, nr) if q < 2 else (own_ref, orow)
                    score = ref[q if q < 2 else 3 - q, pl.ds(row + off, SUB), tile(c)]
                    far_max = row_window(work, q * tiles + c, r + off - base, jnp.maximum)
                    root = far_max == score
                    bits = jnp.where(root, bits | ((31 << q) | (256 << q)), bits)
                    carry = carry + jnp.where(root, 0, 1)
                    behind = jnp.where(root, q + 1, behind)
                for q in (3, 2, 1, 0):
                    ahead = jnp.where((bits & (256 << q)) != 0, 4 - q, ahead)
                bits_out[pl.ds(r + off - lo, SUB), tile(c)] = bits
                to_far.append(ahead)
                to_mate.append(behind)
            rows = pl.ds(pl.multiple_of(r - lo, 2 * SUB), 2 * SUB)
            far_out[rows, tile(c)] = jnp.concatenate(to_far, axis=0).astype(jnp.int16)
            mate_out[rows, tile(c)] = jnp.concatenate(to_mate, axis=0).astype(jnp.int16)
        return carry

    count_out[...] = for_rows(lo, hi, 2 * SUB, (near,), decide, jnp.zeros((SUB, LANES), I32))


def find_roots(where, lo, hi, starts, far, near, own, mate):
    height, width = own.shape[1:]
    tiles = width // LANES
    full = lambda n: [pl.BlockSpec(memory_space=VMEM)] * n
    return pl.pallas_call(
        functools.partial(roots_kernel, spec=(lo, hi, height, tiles, starts, len(far))),
        in_specs=[pl.BlockSpec(memory_space=pltpu.SMEM), *full(len(far) + len(near) + 2)],
        out_specs=full(4),
        out_shape=[
            jax.ShapeDtypeStruct((hi - lo, width), I32),
            jax.ShapeDtypeStruct((hi - lo, width), jnp.int16),
            jax.ShapeDtypeStruct((hi - lo, width), jnp.int16),
            jax.ShapeDtypeStruct((SUB, LANES), I32),
        ],
        scratch_shapes=[VMEM((4 * tiles, hi - lo + 4 * SUB, LANES), I32)],
    )(where, *far, *near, own, mate)


def finish_kernel(where, *args, spec):
    lo, hi, known, height, tiles, starts, n_far, cuts, last_call, n_counts = spec
    args = list(args)
    take = lambda n: [args.pop(0) for _ in range(n)]
    far, near = Rows(starts[:n_far], take(n_far)), Rows(starts, take(len(starts)))
    own, mate = Rows((0,), take(1)), Rows((0,), take(1))
    n = len(cuts)
    bits, ahead, behind = Rows(cuts, take(n)), Rows(cuts, take(n)), Rows(cuts, take(n))
    counts_in = take(n_counts)
    if lo > 0:
        take(1)
    status_out, count_out, reach, gone, work, status, sems = args
    odd, void = where[0], where[1]

    r_lo, r_hi = max(lo - 2 * SUB, 0), known
    w_lo, w_hi = max(lo - SUB, 0), min(hi + SUB, height)
    base = lo - 4 * SUB
    zero = jnp.zeros((SUB, LANES), I32)
    for c in range(tiles):
        if lo == 0:
            reach[c, pl.ds(-SUB - base, SUB), :] = zero
        if known == height:
            reach[c, pl.ds(height - base, SUB), :] = zero
    for k in range(4 * tiles):
        if lo == 0:
            work[k, pl.ds(-SUB - base, SUB), :] = zero - 1
        if hi == height:
            work[k, pl.ds(height - base, SUB), :] = zero - 1

    def dilate(r, pick, carry):
        (b_ref, br), (a_ref, ar), (m_ref, mr) = pick(bits), pick(ahead), pick(behind)
        halves = [[], []]
        for c in range(tiles):
            rows = lambda row: pl.ds(pl.multiple_of(row, 2 * SUB), 2 * SUB)
            from_far = a_ref[rows(ar), tile(c)].astype(I32)
            from_mate = m_ref[rows(mr), tile(c)].astype(I32)
            both = ((1 << from_far) - 1) | (256 - (256 >> from_mate))
            both = both | b_ref[rows(br), tile(c)]
            for half in range(2):
                halves[half].append(both[half * SUB : (half + 1) * SUB])
        for half in range(2):
            wide = lane_window(halves[half], jnp.bitwise_or, 0)
            for c in range(tiles):
                reach[c, pl.ds(r + half * SUB - base, SUB), :] = wide[c]
        return carry

    for_rows(r_lo, r_hi, 2 * SUB, (bits,), dilate)

    def spread(r, pick, carry):
        per_tile = []
        for c in range(tiles):
            removed = row_window(reach, c, r - base, jnp.bitwise_or)
            gone[c, pl.ds(r - base, SUB), :] = removed
            planes = load_planes(pick, far, near, own, mate, 0, c, void)
            left = [
                jnp.where((removed & (1 << k)) != 0, -1, plane) for k, plane in enumerate(planes)
            ]
            per_tile.append(depth_maxima(left))
        for q in range(4):
            wide = lane_window([t[q] for t in per_tile], jnp.maximum, -1)
            for c in range(tiles):
                work[q * tiles + c, pl.ds(r - base, SUB), :] = wide[c]
        return carry

    for_rows(w_lo, w_hi, SUB, (far, near), spread)

    def decide(r, pick, carry):
        near_ref, nr = pick(near)
        own_ref, orow = pick(own)
        b_ref, br = pick(bits)
        second, third = carry
        for c in range(tiles):
            removed = gone[c, pl.ds(r - base, SUB), :]
            first_roots = b_ref[pl.ds(br, SUB), tile(c)]
            for q in range(4):
                ref, row = (near_ref, nr) if q < 2 else (own_ref, orow)
                score = ref[q if q < 2 else 3 - q, pl.ds(row, SUB), tile(c)]
                far_max = row_window(work, q * tiles + c, r - base, jnp.maximum)
                out = (removed & (4 << q)) != 0
                root = (first_roots & (256 << q)) != 0
                second = second + jnp.where(out, 0, 1)
                rest = jnp.where(far_max == score, 1, 0)
                third = third + jnp.where(out, 0, 1 - rest)
                status[q, pl.ds(r - lo, SUB), tile(c)] = jnp.where(
                    root, 1, jnp.where(out, 2, rest)
                )
        return second, third

    copies = []
    carry = (zero, zero)
    steps = [lo, *[s for s in range(0, height, 128) if lo < s < hi], hi]
    for k, (a, b) in enumerate(zip(steps, steps[1:])):
        carry = for_rows(a, b, SUB, (near, bits), decide, carry)
        for q in range(4):
            copies.append(
                pltpu.make_async_copy(
                    status.at[q, pl.ds(a - lo, b - a), :],
                    status_out.at[q + odd * (3 - 2 * q), pl.ds(a, b - a), :],
                    sems.at[4 * k + q],
                )
            )
            copies[-1].start()
    sums = [jnp.sum(t, axis=0, keepdims=True) for t in carry]
    if last_call:
        first = counts_in[0][...]
        for ref in counts_in[1:n]:
            first = first + ref[...]
        rows = [jnp.sum(first, axis=0, keepdims=True), *sums]
        row = lax.broadcasted_iota(I32, (SUB, LANES), 0)
        total = jnp.zeros((SUB, LANES), I32)
        for k in range(3):
            total = jnp.where(row == k, rows[k], total)
        for ref in counts_in[n:]:
            total = total + ref[...]
        count_out[...] = total
    else:
        row = lax.broadcasted_iota(I32, (SUB, LANES), 0)
        total = jnp.zeros((SUB, LANES), I32)
        for k in range(2):
            total = jnp.where(row == k + 1, sums[k], total)
        count_out[...] = total
    for c in copies:
        c.wait()


def finish(where, lo, hi, known, starts, cuts, far, near, own, mate, bits, ahead, behind, counts, status):
    height, width = own.shape[1:]
    tiles = width // LANES
    last_call = hi == height
    full = lambda n: [pl.BlockSpec(memory_space=VMEM)] * n
    args = [*far, *near, own, mate, *bits, *ahead, *behind, *counts]
    in_specs = [pl.BlockSpec(memory_space=pltpu.SMEM), *full(len(args))]
    aliases = {}
    if lo > 0:
        args.append(status)
        in_specs.append(pl.BlockSpec(memory_space=pl.ANY))
        aliases = {len(args): 0}
    span = hi - lo + 6 * SUB
    steps = (hi - lo + 127) // 128 + 1
    return pl.pallas_call(
        functools.partial(
            finish_kernel,
            spec=(lo, hi, known, height, tiles, starts, len(far), cuts, last_call, len(counts)),
        ),
        in_specs=in_specs,
        out_specs=[pl.BlockSpec(memory_space=pl.ANY), pl.BlockSpec(memory_space=VMEM)],
        out_shape=[
            jax.ShapeDtypeStruct((4, height, width), I32),
            jax.ShapeDtypeStruct((SUB, LANES), I32),
        ],
        scratch_shapes=[
            VMEM((tiles, span, LANES), I32),
            VMEM((tiles, span, LANES), I32),
            VMEM((4 * tiles, span, LANES), I32),
            VMEM((4, hi - lo, width), I32),
            pltpu.SemaphoreType.DMA((4 * steps,)),
        ],
        input_output_aliases=aliases,
    )(where, *args)


def pairs(count, swap):
    return [(i, swap(i)) for i in range(count) if 0 <= swap(i) < count]


def total_over_slice(part):
    count = lax.axis_size(GZ)
    for scale, turn in ((1, 1), (2, 1), (2, 3), (8, 1), (8, 3), (32, 1), (32, 3)):
        part = part + lax.ppermute(part, GZ, pairs(count, lambda i: i ^ (scale * turn)))
    return part


def shards(scores):
    count = lax.axis_size(GZ)
    height = scores.shape[1]
    me = lax.axis_index(GZ)
    odd = me % 2
    edge = (me == 0) | (me == count - 1)
    where = jnp.stack([odd, jnp.where(edge, -1, 0)]).astype(I32)
    over = lambda x: lax.ppermute(x, GZ, pairs(count, lambda i: i - 1 + 2 * (i % 2)))
    swap = lambda x: lax.ppermute(x, GZ, pairs(count, lambda i: i ^ 1))

    starts = (0, *CUTS)
    ends = (*CUTS, height)
    root_ends = (*[c - 2 * SUB for c in CUTS], height)
    final_ends = (*[c - 4 * SUB for c in CUTS], height)
    near = [*cut(where, scores, (("near", 0, ends[0]),))]
    far = [over(near[0])]
    *more, own = cut(
        where, scores, (*[("near", a, b) for a, b in zip(starts[1:], ends[1:])], ("own", 0, height))
    )
    near += more
    far += [over(x) for x in more]
    mate = swap(own)

    bits, ahead, behind, counts = [], [], [], []
    cuts = (0, *root_ends[:-1])
    for k, (lo, hi) in enumerate(zip(cuts, root_ends)):
        b, a, m, c = find_roots(where, lo, hi, starts, far[: k + 1], near, own, mate)
        bits.append(b)
        counts.append(c)
        ahead.append(over(a))
        behind.append(swap(m))
    status, later = None, []
    finals = (0, *final_ends[:-1])
    for k, (lo, hi) in enumerate(zip(finals, final_ends)):
        status, c = finish(
            where, lo, hi, root_ends[k], starts, cuts[: k + 1], far[: k + 1], near, own, mate,
            bits[: k + 1], ahead[: k + 1], behind[: k + 1],
            [*counts, *later] if hi == height else [], status,
        )
        later.append(c)
    total = total_over_slice(later[-1])
    return status, jnp.sum(total[:3], axis=1)


def solution(mesh):
    finer = Mesh(mesh.devices.reshape(4, 4, 4, 2), GZ)
    return jax.shard_map(
        shards, mesh=finer, in_specs=(P(GZ, None, None),), out_specs=(P(GZ, None, None), P()),
        check_vma=False,
    )
```

```python
import functools

import jax
import jax.numpy as jnp
from jax import lax
from jax.experimental import pallas as pl
from jax.experimental.pallas import tpu as pltpu
from jax.sharding import Mesh
from jax.sharding import PartitionSpec as P


GZ = ("gz_0", "gz_1", "gz_2", "gz_3")
LANES = 128
SUB = 8
VMEM = pltpu.VMEM
I32 = jnp.int32
U32 = jnp.int32
GRANT = pltpu.CompilerParams(vmem_limit_bytes=30 << 20)

EARLY = 3
BOX = 4


def in_vmem(x):
    return pltpu.with_memory_space_constraint(x, VMEM)


def smem():
    return pl.BlockSpec(memory_space=pltpu.SMEM)


def vmem(n):
    return [pl.BlockSpec(memory_space=VMEM)] * n


class Rows:
    def __init__(self, starts, refs):
        self.starts, self.refs = starts, refs

    def at(self, row):
        k = max(i for i, s in enumerate(self.starts) if s <= row)
        return self.refs[k], self.starts[k]


def for_rows(lo, hi, step, sources, body, unroll=1):
    edges = sorted({lo, hi, *[e for s in sources for e in s.starts if lo < e < hi]})
    for a, b in zip(edges, edges[1:]):
        def some(i, c, times, first, a=a):
            for u in range(times):
                r = first + (i * times + u) * step
                pick = lambda rows, r=r: (
                    rows.at(a)[0], pl.multiple_of(r - rows.at(a)[1], SUB)
                )
                body(r if isinstance(r, int) else pl.multiple_of(r, SUB), pick)
            return c

        groups = (b - a) // step
        whole = groups // unroll
        if whole:
            lax.fori_loop(0, whole, functools.partial(some, times=unroll, first=a), 0)
        if groups % unroll:
            some(0, 0, groups % unroll, a + whole * unroll * step)


def tile(c):
    return pl.ds(c * LANES, LANES)


def window(ref, index, first, count, op):
    out = ref[index, pl.ds(first - 2, count), :]
    for k in (-1, 0, 1, 2):
        out = op(out, ref[index, pl.ds(first + k, count), :])
    return out


def depth_maxima(p):
    mid = jnp.maximum(p[3], p[4])
    low = jnp.maximum(p[2], mid)
    all4 = jnp.maximum(low, p[5])
    return (
        jnp.maximum(low, jnp.maximum(p[0], p[1])),
        jnp.maximum(all4, p[1]),
        jnp.maximum(all4, p[6]),
        jnp.maximum(jnp.maximum(mid, p[5]), jnp.maximum(p[6], p[7])),
    )


def load_planes(pick, far, near, own, mate, c, inside):
    f, fr = pick(far)
    n, nr = pick(near)
    o, orow = pick(own)
    m, mr = pick(mate)
    get = lambda ref, k, r: ref[k, pl.ds(r, SUB), tile(c)].astype(U32)
    return [
        get(f, 1, fr) & inside,
        get(f, 0, fr) & inside,
        get(n, 0, nr),
        get(n, 1, nr),
        get(o, 1, orow),
        get(o, 0, orow),
        get(m, 0, mr),
        get(m, 1, mr),
    ]


def inside_mask(where):
    return jnp.full((SUB, LANES), where[1], I32).astype(U32)


def clear(ref, index, row):
    ref[index, pl.ds(row, SUB), :] = jnp.zeros((SUB, LANES), ref.dtype)


def cut_kernel(where, scores, *rest, parts, after):
    rest = rest[after:]
    outs, sems = rest[: len(parts)], rest[len(parts)]
    odd = where[0]
    copies = []
    for out, (kind, lo, hi) in zip(outs, parts):
        for k in range(2):
            j = k if kind == "near" else 3 - k
            plane = j + odd * (3 - 2 * j)
            copies.append(
                pltpu.make_async_copy(
                    scores.at[plane, pl.ds(lo, hi - lo), :], out.at[k], sems.at[len(copies)]
                )
            )
    for c in copies:
        c.start()
    for c in copies:
        c.wait()


def cut(where, scores, parts, after=()):
    width = scores.shape[2]
    return pl.pallas_call(
        functools.partial(cut_kernel, parts=parts, after=len(after)),
        compiler_params=GRANT,
        in_specs=[smem(), *[pl.BlockSpec(memory_space=pl.ANY)] * (1 + len(after))],
        out_specs=vmem(len(parts)),
        out_shape=[VMEM((2, hi - lo, width), I32) for _, lo, hi in parts],
        scratch_shapes=[pltpu.SemaphoreType.DMA((2 * len(parts),))],
    )(where, scores, *after)


def turn_kernel(*args, starts, height, tiles):
    near, own, out = Rows(starts, args[: len(starts)]), args[len(starts)], args[-1]
    for q in range(4):
        def body(b, carry, q=q):
            for c in range(tiles):
                rows = pl.ds(pl.multiple_of(b * LANES, LANES), LANES)
                block = own[3 - q, rows, tile(c)]
                out[q, b, pl.ds(c * LANES, LANES), :] = block.T
            return carry

        if q >= 2:
            lax.fori_loop(0, height // LANES, body, 0)
            continue
        for b in range(height // LANES):
            for c in range(tiles):
                pieces = []
                for s, e in zip(starts, (*starts[1:], height)):
                    lo, hi = max(s, b * LANES), min(e, (b + 1) * LANES)
                    if lo < hi:
                        pieces.append(near.at(lo)[0][q, pl.ds(lo - s, hi - lo), tile(c)])
                block = pieces[0] if len(pieces) == 1 else jnp.concatenate(pieces, axis=0)
                out[q, b, pl.ds(c * LANES, LANES), :] = block.T


def turn(starts, near, own):
    height, width = own.shape[1:]
    args = [in_vmem(x) for x in (*near, own)]
    return pl.pallas_call(
        functools.partial(turn_kernel, starts=starts, height=height, tiles=width // LANES),
        compiler_params=GRANT,
        in_specs=vmem(len(args)),
        out_specs=vmem(1)[0],
        out_shape=VMEM((4, height // LANES, width, LANES), I32),
    )(*args)


def box_columns(maxima, columns, first, tiles):
    def body(k, carry):
        wide = window(maxima, k, first, LANES, jnp.maximum)
        at = pl.multiple_of((k % tiles) * LANES, LANES) + SUB
        columns[k // tiles, pl.ds(at, LANES), :] = wide.T
        return carry

    lax.fori_loop(0, 4 * tiles, body, 0, unroll=BOX)


def roots_kernel(where, *args, spec):
    first, last, height, width, starts, n_far, n_before = spec
    tiles = width // LANES
    args = list(args)
    take = lambda n: [args.pop(0) for _ in range(n)]
    far, near = Rows(starts[:n_far], take(n_far)), Rows(starts, take(len(starts)))
    own, mate = Rows((0,), take(1)), Rows((0,), take(1))
    (turned,) = take(1)
    take(n_before)
    bits_out, far_out, mate_out, maxima, columns = args
    inside = inside_mask(where)
    lo, hi = first * LANES, last * LANES
    base = lo - SUB

    for k in range(4 * tiles):
        if lo == 0:
            clear(maxima, k, 0)
        if hi == height:
            clear(maxima, k, hi - base)
    for q in range(4):
        clear(columns, q, 0)
        clear(columns, q, SUB + width)

    def spread(r, pick):
        for c in range(tiles):
            deep = depth_maxima(load_planes(pick, far, near, own, mate, c, inside))
            for q in range(4):
                maxima[q * tiles + c, pl.ds(r - base, SUB), :] = deep[q]

    for_rows(max(lo - SUB, 0), min(hi + SUB, height), SUB, (far, near), spread, 2)

    for b in range(first, last):
        box_columns(maxima, columns, b * LANES - base, tiles)

        def decide(i, carry, b=b):
            at = pl.multiple_of(i * 2 * SUB, 2 * SUB)
            to_far, to_mate = [], []
            for half in range(2):
                bits = jnp.zeros((SUB, LANES), I32)
                ahead = behind = bits
                found = []
                for q in range(4):
                    box = window(columns, q, at + (half + 1) * SUB, SUB, jnp.maximum)
                    score = turned[q, b, pl.ds(at + half * SUB, SUB), :].astype(U32)
                    found.append(box == score)
                for q in range(4):
                    behind = jnp.where(found[q], q + 1, behind)
                    ahead = jnp.where(found[3 - q], q + 1, ahead)
                    bits = jnp.where(found[q], bits | ((31 << q) | (256 << q)), bits)
                bits_out[b, pl.ds(at + half * SUB, SUB), :] = bits
                to_far.append(ahead)
                to_mate.append(behind)
            both = pl.ds(at, 2 * SUB)
            far_out[b, both, :] = jnp.concatenate(to_far, axis=0).astype(jnp.int16)
            mate_out[b, both, :] = jnp.concatenate(to_mate, axis=0).astype(jnp.int16)
            return carry

        lax.fori_loop(0, width // (2 * SUB), decide, 0)


def find_roots(where, first, last, starts, far, near, own, mate, turned, before):
    height, width = own.shape[1:]
    args = [in_vmem(x) for x in (*far, *near, own, mate, turned, *before)]
    blocks = last - first
    shape = (height // LANES, width, LANES)
    spec = (first, last, height, width, starts, len(far), len(before))
    n = len(args) + 1 - len(before)
    return pl.pallas_call(
        functools.partial(roots_kernel, spec=spec),
        compiler_params=GRANT,
        in_specs=[smem(), *vmem(len(args))],
        out_specs=vmem(3),
        out_shape=[VMEM(shape, I32), VMEM(shape, jnp.int16), VMEM(shape, jnp.int16)],
        scratch_shapes=[
            VMEM((4 * width // LANES, blocks * LANES + 2 * SUB, LANES), U32),
            VMEM((4, width + 2 * SUB, LANES), U32),
        ],
        input_output_aliases={n + k: k for k in range(len(before))},
    )(where, *args)


def finish_kernel(where, *args, spec):
    height, width, starts = spec
    tiles, blocks = width // LANES, height // LANES
    args = list(args)
    take = lambda n: [args.pop(0) for _ in range(n)]
    far, near = Rows(starts, take(len(starts))), Rows(starts, take(len(starts)))
    own, mate = Rows((0,), take(1)), Rows((0,), take(1))
    (turned,) = take(1)
    bits, ahead, behind = take(3)
    status_out, count_out, reach, spots, gone, maxima, columns, marks, turned_marks, status, sems = args
    inside = inside_mask(where)
    odd = where[0]

    for k in range(4 * tiles):
        clear(maxima, k, 0)
        clear(maxima, k, SUB + height)
    for k in range(4):
        clear(columns, k, 0)
        clear(columns, k, SUB + width)
    for b in range(blocks):
        clear(reach, b, 0)
        clear(reach, b, SUB + width)
    for c in range(tiles):
        clear(spots, c, 0)
        clear(spots, c, SUB + height)

    def gather(i, carry):
        both = pl.ds(pl.multiple_of(i * 2 * SUB, 2 * SUB), 2 * SUB)
        for b in range(blocks):
            from_far = ahead[b, both, :].astype(I32)
            from_mate = behind[b, both, :].astype(I32)
            out = ((1 << from_far) - 1) | (256 - (256 >> from_mate)) | bits[b, both, :]
            reach[b, pl.ds(pl.multiple_of(i * 2 * SUB + SUB, SUB), 2 * SUB), :] = out
        return carry

    lax.fori_loop(0, width // (2 * SUB), gather, 0)

    def turn_back(b, carry):
        at = pl.multiple_of(SUB + b * LANES, SUB)
        for c in range(tiles):
            wide = window(reach, b, SUB + c * LANES, LANES, jnp.bitwise_or)
            spots[c, pl.ds(at, LANES), :] = wide.T
        return carry

    lax.fori_loop(0, blocks, turn_back, 0)

    def spread(r, pick):
        for c in range(tiles):
            removed = window(spots, c, r + SUB, SUB, jnp.bitwise_or)
            gone[c, pl.ds(r, SUB), :] = removed
            planes = load_planes(pick, far, near, own, mate, c, inside)
            left = [
                jnp.where((removed & (1 << k)) != 0, jnp.zeros_like(plane), plane)
                for k, plane in enumerate(planes)
            ]
            deep = depth_maxima(left)
            for q in range(4):
                maxima[q * tiles + c, pl.ds(r + SUB, SUB), :] = deep[q]

    for_rows(0, height, SUB, (far, near), spread, 2)

    copies = []
    zero = jnp.zeros((SUB, LANES), I32)
    carry = (zero, zero, zero)
    for b in range(blocks):
        box_columns(maxima, columns, SUB + b * LANES, tiles)

        def decide(i, c, b=b):
            at = pl.multiple_of(i * SUB, SUB)
            out = bits[b, pl.ds(at, SUB), :] & (15 << 8)
            for q in range(4):
                box = window(columns, q, at + SUB, SUB, jnp.maximum)
                score = turned[q, b, pl.ds(at, SUB), :].astype(U32)
                out = jnp.where(box == score, out | (1 << q), out)
            marks[pl.ds(at, SUB), :] = out
            return c

        lax.fori_loop(0, width // SUB, decide, 0, unroll=2)
        for c in range(tiles):
            turned_marks[c] = marks[pl.ds(c * LANES, LANES), :].T

        def settle(i, sums, b=b):
            at = pl.multiple_of(i * SUB, SUB)
            one, two, three = sums
            for c in range(tiles):
                mark = turned_marks[c, pl.ds(at, SUB), :]
                out = (gone[c, pl.ds(b * LANES + at, SUB), :] >> 2) & 15
                root = mark >> 8
                late = mark & 15 & ~out
                one = one + lax.population_count(root)
                two = two + lax.population_count(out)
                three = three + lax.population_count(out | late)
                ones, twos = root | late, out & ~root
                for q in range(4):
                    state = ((ones >> q) & 1) | (((twos << 1) >> q) & 2)
                    status[q, pl.ds(b * LANES + at, SUB), tile(c)] = state
            return one, two, three

        carry = lax.fori_loop(0, LANES // SUB, settle, carry)
        for q in range(4):
            copies.append(
                pltpu.make_async_copy(
                    status.at[q, pl.ds(b * LANES, LANES), :],
                    status_out.at[q + odd * (3 - 2 * q), pl.ds(b * LANES, LANES), :],
                    sems.at[4 * b + q],
                )
            )
            copies[-1].start()
    lane = lax.broadcasted_iota(I32, (1, LANES), 1)
    total = jnp.zeros((1, LANES), I32)
    for k in range(3):
        total = jnp.where(lane == k, 4 * height * width - jnp.sum(carry[k]), total)
    count_out[...] = jnp.broadcast_to(total, count_out.shape)
    for c in copies:
        c.wait()


def finish(where, starts, far, near, own, mate, turned, bits, ahead, behind, fan):
    height, width = own.shape[1:]
    tiles, blocks = width // LANES, height // LANES
    args = [in_vmem(x) for x in (*far, *near, own, mate, turned, bits, ahead, behind)]
    return pl.pallas_call(
        functools.partial(finish_kernel, spec=(height, width, starts)),
        compiler_params=GRANT,
        in_specs=[smem(), *vmem(len(args))],
        out_specs=[pl.BlockSpec(memory_space=pl.ANY), vmem(1)[0]],
        out_shape=[
            jax.ShapeDtypeStruct((4, height, width), I32),
            VMEM((fan, LANES), I32),
        ],
        scratch_shapes=[
            VMEM((blocks, width + 2 * SUB, LANES), I32),
            VMEM((tiles, height + 2 * SUB, LANES), I32),
            VMEM((tiles, height, LANES), I32),
            VMEM((4 * tiles, height + 2 * SUB, LANES), U32),
            VMEM((4, width + 2 * SUB, LANES), U32),
            VMEM((width, LANES), I32),
            VMEM((tiles, LANES, LANES), I32),
            VMEM((4, height, width), I32),
            pltpu.SemaphoreType.DMA((4 * blocks,)),
        ],
    )(where, *args)


def pairs(count, swap):
    return [(i, swap(i)) for i in range(count) if 0 <= swap(i) < count]


def shards(scores):
    count = lax.axis_size(GZ)
    height = scores.shape[1]
    blocks = height // LANES
    me = lax.axis_index(GZ)
    odd = me % 2
    edge = (me == 0) | (me == count - 1)
    where = jnp.stack([odd, jnp.where(edge, 0, -1)]).astype(I32)
    over = lambda x: lax.ppermute(x, GZ, pairs(count, lambda i: i - 1 + 2 * (i % 2)))
    swap = lambda x: lax.ppermute(x, GZ, pairs(count, lambda i: i ^ 1))

    early = EARLY if 0 < EARLY < blocks else 0
    starts = (0, early * LANES + SUB) if early else (0,)
    ends = (*starts[1:], height)
    firsts = (0, early) if early else (0,)
    lasts = (*firsts[1:], blocks)

    scores = pltpu.with_memory_space_constraint(scores, pltpu.HBM)
    near = [*cut(where, scores, (("near", 0, ends[0]),))]
    far = [over(near[0])]
    rest = [("near", a, b) for a, b in zip(starts[1:], ends[1:])]
    *more, own = cut(where, scores, (*rest, ("own", 0, height)), (in_vmem(near[0]),))
    near += more
    far += [over(x) for x in more]
    mate = swap(own)
    turned = turn(starts, near, own)

    found = ()
    for k, (a, b) in enumerate(zip(firsts, lasts)):
        found = find_roots(
            where, a, b, starts, far[: k + 1], near, own, mate, turned, found
        )
    bits, ahead, behind = found
    status, part = finish(
        where, starts, far, near, own, mate, turned, bits, over(ahead), swap(behind), count
    )
    total = jnp.sum(lax.all_to_all(part, GZ, 0, 0, tiled=True), axis=0)
    return status, total[:3]


def solution(mesh):
    finer = Mesh(mesh.devices.reshape(4, 4, 4, 2), GZ)
    return jax.shard_map(
        shards, mesh=finer, in_specs=(P(GZ, None, None),), out_specs=(P(GZ, None, None), P()),
        check_vma=False,
    )
```

```python
import functools

import jax
import jax.numpy as jnp
from jax import lax
from jax.experimental import pallas as pl
from jax.experimental.pallas import tpu as pltpu
from jax.sharding import Mesh
from jax.sharding import PartitionSpec as P


GZ = ("gz_0", "gz_1", "gz_2", "gz_3")
LANES = 128
SUB = 8
VMEM = pltpu.VMEM
I32 = jnp.int32
U32 = jnp.int32
GRANT = pltpu.CompilerParams(vmem_limit_bytes=30 << 20)

EARLY = 3
SCORE_BITS = 27
SPARE = 32 - SCORE_BITS
BOX = 16


def in_vmem(x):
    return pltpu.with_memory_space_constraint(x, VMEM)


def smem():
    return pl.BlockSpec(memory_space=pltpu.SMEM)


def vmem(n):
    return [pl.BlockSpec(memory_space=VMEM)] * n


class Rows:
    def __init__(self, starts, refs):
        self.starts, self.refs = starts, refs

    def at(self, row):
        k = max(i for i, s in enumerate(self.starts) if s <= row)
        return self.refs[k], self.starts[k]


def for_rows(lo, hi, step, sources, body, unroll=1):
    edges = sorted({lo, hi, *[e for s in sources for e in s.starts if lo < e < hi]})
    for a, b in zip(edges, edges[1:]):
        def some(i, c, times, first, a=a):
            for u in range(times):
                r = first + (i * times + u) * step
                pick = lambda rows, r=r: (
                    rows.at(a)[0], pl.multiple_of(r - rows.at(a)[1], SUB)
                )
                body(r if isinstance(r, int) else pl.multiple_of(r, SUB), pick)
            return c

        groups = (b - a) // step
        whole = groups // unroll
        if whole:
            lax.fori_loop(0, whole, functools.partial(some, times=unroll, first=a), 0)
        if groups % unroll:
            some(0, 0, groups % unroll, a + whole * unroll * step)


def tile(c):
    return pl.ds(c * LANES, LANES)


def window(ref, index, first, count, op):
    out = ref[index, pl.ds(first - 2, count), :]
    for k in (-1, 0, 1, 2):
        out = op(out, ref[index, pl.ds(first + k, count), :])
    return out


def depth_maxima(p):
    mid = jnp.maximum(p[3], p[4])
    low = jnp.maximum(p[2], mid)
    all4 = jnp.maximum(low, p[5])
    return (
        jnp.maximum(low, jnp.maximum(p[0], p[1])),
        jnp.maximum(all4, p[1]),
        jnp.maximum(all4, p[6]),
        jnp.maximum(jnp.maximum(mid, p[5]), jnp.maximum(p[6], p[7])),
    )


def load_planes(pick, far, near, own, mate, c, inside):
    f, fr = pick(far)
    n, nr = pick(near)
    o, orow = pick(own)
    m, mr = pick(mate)
    get = lambda ref, k, r: ref[k, pl.ds(r, SUB), tile(c)].astype(U32)
    return [
        get(f, 1, fr) & inside,
        get(f, 0, fr) & inside,
        get(n, 0, nr),
        get(n, 1, nr),
        get(o, 1, orow),
        get(o, 0, orow),
        get(m, 0, mr),
        get(m, 1, mr),
    ]


def inside_mask(where):
    return jnp.full((SUB, LANES), where[1], I32).astype(U32)


def clear(ref, index, row):
    ref[index, pl.ds(row, SUB), :] = jnp.zeros((SUB, LANES), ref.dtype)


def packed_rows(rows):
    groups = rows // SUB
    return SUB * (groups - groups // 7)


def for_groups(rows, body):
    whole = rows // SUB // 7

    def one(i, carry):
        body(pl.multiple_of(i * 7 * SUB, SUB), pl.multiple_of(i * 6 * SUB, SUB), True)
        return carry

    if whole:
        lax.fori_loop(0, whole, one, 0)
    for j in range(rows // SUB - 7 * whole):
        body((7 * whole + j) * SUB, (6 * whole + j) * SUB, False)


def pack(src, dst, rows, tiles):
    def body(r, w, whole):
        for k in range(2):
            for c in range(tiles):
                get = lambda j: src[k, pl.ds(r + j * SUB, SUB), tile(c)]
                if not whole:
                    dst[k, pl.ds(w, SUB), tile(c)] = get(0)
                    continue
                last = get(6)
                for j in range(6):
                    part = lax.shift_left(
                        lax.shift_right_logical(last, SPARE * j), SCORE_BITS
                    )
                    dst[k, pl.ds(w + j * SUB, SUB), tile(c)] = get(j) | part

    for_groups(rows, body)


def unpack_kernel(src, *rest, rows, tiles):
    dst = rest[-1]

    def body(r, w, whole):
        for k in range(2):
            for c in range(tiles):
                get = lambda j: src[k, pl.ds(w + j * SUB, SUB), tile(c)]
                if not whole:
                    dst[k, pl.ds(r, SUB), tile(c)] = get(0)
                    continue
                last = jnp.zeros((SUB, LANES), I32)
                for j in range(6):
                    word = get(j)
                    dst[k, pl.ds(r + j * SUB, SUB), tile(c)] = word & ((1 << SCORE_BITS) - 1)
                    part = lax.shift_right_logical(word, SCORE_BITS)
                    last = last | lax.shift_left(part, SPARE * j)
                dst[k, pl.ds(r + 6 * SUB, SUB), tile(c)] = last

    for_groups(rows, body)


def unpack(words, rows, after=()):
    width = words.shape[2]
    return pl.pallas_call(
        functools.partial(unpack_kernel, rows=rows, tiles=width // LANES),
        compiler_params=GRANT,
        in_specs=[*vmem(1), *[pl.BlockSpec(memory_space=pl.ANY)] * len(after)],
        out_specs=vmem(1)[0],
        out_shape=VMEM((2, rows, width), I32),
    )(in_vmem(words), *[in_vmem(x) for x in after])


def cut_kernel(where, scores, *rest, parts, after, tiles):
    rest = rest[after:]
    n_packed = sum(kind == "near" for kind, _, _ in parts)
    outs, packed = rest[: len(parts)], list(rest[len(parts) : len(parts) + n_packed])
    sems = rest[len(parts) + n_packed]
    odd = where[0]
    copies = []
    for out, (kind, lo, hi) in zip(outs, parts):
        for k in range(2):
            j = k if kind == "near" else 3 - k
            plane = j + odd * (3 - 2 * j)
            copies.append(
                pltpu.make_async_copy(
                    scores.at[plane, pl.ds(lo, hi - lo), :], out.at[k], sems.at[len(copies)]
                )
            )
    for c in copies:
        c.start()
    for i, (out, (kind, lo, hi)) in enumerate(zip(outs, parts)):
        copies[2 * i].wait()
        copies[2 * i + 1].wait()
        if kind == "near":
            pack(out, packed.pop(0), hi - lo, tiles)


def cut(where, scores, parts, after=()):
    width = scores.shape[2]
    sent = [hi - lo for kind, lo, hi in parts if kind == "near"]
    out = pl.pallas_call(
        functools.partial(cut_kernel, parts=parts, after=len(after), tiles=width // LANES),
        compiler_params=GRANT,
        in_specs=[smem(), *[pl.BlockSpec(memory_space=pl.ANY)] * (1 + len(after))],
        out_specs=vmem(len(parts) + len(sent)),
        out_shape=[
            *[VMEM((2, hi - lo, width), I32) for _, lo, hi in parts],
            *[VMEM((2, packed_rows(n), width), I32) for n in sent],
        ],
        scratch_shapes=[pltpu.SemaphoreType.DMA((2 * len(parts),))],
    )(where, scores, *after)
    return out[: len(parts)], out[len(parts) :]


def turn_kernel(*args, starts, height, tiles):
    near, own, out = Rows(starts, args[: len(starts)]), args[len(starts)], args[-1]
    for q in range(4):
        def body(b, carry, q=q):
            for c in range(tiles):
                rows = pl.ds(pl.multiple_of(b * LANES, LANES), LANES)
                block = own[3 - q, rows, tile(c)]
                out[q, b, pl.ds(c * LANES, LANES), :] = block.T
            return carry

        if q >= 2:
            lax.fori_loop(0, height // LANES, body, 0)
            continue
        for b in range(height // LANES):
            for c in range(tiles):
                pieces = []
                for s, e in zip(starts, (*starts[1:], height)):
                    lo, hi = max(s, b * LANES), min(e, (b + 1) * LANES)
                    if lo < hi:
                        pieces.append(near.at(lo)[0][q, pl.ds(lo - s, hi - lo), tile(c)])
                block = pieces[0] if len(pieces) == 1 else jnp.concatenate(pieces, axis=0)
                out[q, b, pl.ds(c * LANES, LANES), :] = block.T


def turn(starts, near, own):
    height, width = own.shape[1:]
    args = [in_vmem(x) for x in (*near, own)]
    return pl.pallas_call(
        functools.partial(turn_kernel, starts=starts, height=height, tiles=width // LANES),
        compiler_params=GRANT,
        in_specs=vmem(len(args)),
        out_specs=vmem(1)[0],
        out_shape=VMEM((4, height // LANES, width, LANES), I32),
    )(*args)


def box_columns(maxima, columns, first, tiles):
    def body(k, carry):
        wide = window(maxima, k, first, LANES, jnp.maximum)
        at = pl.multiple_of((k % tiles) * LANES, LANES) + SUB
        columns[k // tiles, pl.ds(at, LANES), :] = wide.T
        return carry

    lax.fori_loop(0, 4 * tiles, body, 0, unroll=BOX)


def roots_kernel(where, *args, spec):
    first, last, height, width, starts, n_far, n_before = spec
    tiles = width // LANES
    args = list(args)
    take = lambda n: [args.pop(0) for _ in range(n)]
    far, near = Rows(starts[:n_far], take(n_far)), Rows(starts, take(len(starts)))
    own, mate = Rows((0,), take(1)), Rows((0,), take(1))
    (turned,) = take(1)
    take(n_before)
    bits_out, far_out, mate_out, maxima, columns = args
    inside = inside_mask(where)
    lo, hi = first * LANES, last * LANES
    base = lo - SUB

    for k in range(4 * tiles):
        if lo == 0:
            clear(maxima, k, 0)
        if hi == height:
            clear(maxima, k, hi - base)
    for q in range(4):
        clear(columns, q, 0)
        clear(columns, q, SUB + width)

    def spread(r, pick):
        for c in range(tiles):
            deep = depth_maxima(load_planes(pick, far, near, own, mate, c, inside))
            for q in range(4):
                maxima[q * tiles + c, pl.ds(r - base, SUB), :] = deep[q]

    for_rows(max(lo - SUB, 0), min(hi + SUB, height), SUB, (far, near), spread, 2)

    for b in range(first, last):
        box_columns(maxima, columns, b * LANES - base, tiles)

        def decide(i, carry, b=b):
            at = pl.multiple_of(i * 2 * SUB, 2 * SUB)
            to_far, to_mate = [], []
            for half in range(2):
                bits = jnp.zeros((SUB, LANES), I32)
                ahead = behind = bits
                found = []
                for q in range(4):
                    box = window(columns, q, at + (half + 1) * SUB, SUB, jnp.maximum)
                    score = turned[q, b, pl.ds(at + half * SUB, SUB), :].astype(U32)
                    found.append(box == score)
                for q in range(4):
                    behind = jnp.where(found[q], q + 1, behind)
                    ahead = jnp.where(found[3 - q], q + 1, ahead)
                    bits = jnp.where(found[q], bits | ((31 << q) | (256 << q)), bits)
                bits_out[b, pl.ds(at + half * SUB, SUB), :] = bits
                to_far.append(ahead)
                to_mate.append(behind)
            both = pl.ds(at, 2 * SUB)
            far_out[b, both, :] = jnp.concatenate(to_far, axis=0).astype(jnp.int16)
            mate_out[b, both, :] = jnp.concatenate(to_mate, axis=0).astype(jnp.int16)
            return carry

        lax.fori_loop(0, width // (2 * SUB), decide, 0, unroll=2)


def find_roots(where, first, last, starts, far, near, own, mate, turned, before):
    height, width = own.shape[1:]
    args = [in_vmem(x) for x in (*far, *near, own, mate, turned, *before)]
    blocks = last - first
    shape = (height // LANES, width, LANES)
    spec = (first, last, height, width, starts, len(far), len(before))
    n = len(args) + 1 - len(before)
    return pl.pallas_call(
        functools.partial(roots_kernel, spec=spec),
        compiler_params=GRANT,
        in_specs=[smem(), *vmem(len(args))],
        out_specs=vmem(3),
        out_shape=[VMEM(shape, I32), VMEM(shape, jnp.int16), VMEM(shape, jnp.int16)],
        scratch_shapes=[
            VMEM((4 * width // LANES, blocks * LANES + 2 * SUB, LANES), U32),
            VMEM((4, width + 2 * SUB, LANES), U32),
        ],
        input_output_aliases={n + k: k for k in range(len(before))},
    )(where, *args)


def finish_kernel(where, *args, spec):
    height, width, starts = spec
    tiles, blocks = width // LANES, height // LANES
    args = list(args)
    take = lambda n: [args.pop(0) for _ in range(n)]
    far, near = Rows(starts, take(len(starts))), Rows(starts, take(len(starts)))
    own, mate = Rows((0,), take(1)), Rows((0,), take(1))
    (turned,) = take(1)
    bits, ahead, behind = take(3)
    status_out, count_out, reach, spots, gone, maxima, columns, marks, turned_marks, status, sems = args
    inside = inside_mask(where)
    odd = where[0]

    for k in range(4 * tiles):
        clear(maxima, k, 0)
        clear(maxima, k, SUB + height)
    for k in range(4):
        clear(columns, k, 0)
        clear(columns, k, SUB + width)
    for b in range(blocks):
        clear(reach, b, 0)
        clear(reach, b, SUB + width)
    for c in range(tiles):
        clear(spots, c, 0)
        clear(spots, c, SUB + height)

    def gather(i, carry):
        both = pl.ds(pl.multiple_of(i * 2 * SUB, 2 * SUB), 2 * SUB)
        for b in range(blocks):
            from_far = ahead[b, both, :].astype(I32)
            from_mate = behind[b, both, :].astype(I32)
            out = ((1 << from_far) - 1) | (256 - (256 >> from_mate)) | bits[b, both, :]
            reach[b, pl.ds(pl.multiple_of(i * 2 * SUB + SUB, SUB), 2 * SUB), :] = out
        return carry

    lax.fori_loop(0, width // (2 * SUB), gather, 0, unroll=2)

    def turn_back(b, carry):
        at = pl.multiple_of(SUB + b * LANES, SUB)
        for c in range(tiles):
            wide = window(reach, b, SUB + c * LANES, LANES, jnp.bitwise_or)
            spots[c, pl.ds(at, LANES), :] = wide.T
        return carry

    lax.fori_loop(0, blocks, turn_back, 0, unroll=2)

    def spread(r, pick):
        for c in range(tiles):
            removed = window(spots, c, r + SUB, SUB, jnp.bitwise_or)
            gone[c, pl.ds(r, SUB), :] = removed
            planes = load_planes(pick, far, near, own, mate, c, inside)
            left = [
                jnp.where((removed & (1 << k)) != 0, jnp.zeros_like(plane), plane)
                for k, plane in enumerate(planes)
            ]
            deep = depth_maxima(left)
            for q in range(4):
                maxima[q * tiles + c, pl.ds(r + SUB, SUB), :] = deep[q]

    for_rows(0, height, SUB, (far, near), spread, 2)

    copies = []
    zero = jnp.zeros((SUB, LANES), I32)
    carry = (zero, zero, zero)
    for b in range(blocks):
        box_columns(maxima, columns, SUB + b * LANES, tiles)

        def decide(i, c, b=b):
            at = pl.multiple_of(i * SUB, SUB)
            out = bits[b, pl.ds(at, SUB), :] & (15 << 8)
            for q in range(4):
                box = window(columns, q, at + SUB, SUB, jnp.maximum)
                score = turned[q, b, pl.ds(at, SUB), :].astype(U32)
                out = jnp.where(box == score, out | (1 << q), out)
            marks[pl.ds(at, SUB), :] = out
            return c

        lax.fori_loop(0, width // SUB, decide, 0, unroll=4)
        for c in range(tiles):
            turned_marks[c] = marks[pl.ds(c * LANES, LANES), :].T

        def settle(i, sums, b=b):
            at = pl.multiple_of(i * SUB, SUB)
            one, two, three = sums
            for c in range(tiles):
                mark = turned_marks[c, pl.ds(at, SUB), :]
                out = (gone[c, pl.ds(b * LANES + at, SUB), :] >> 2) & 15
                root = mark >> 8
                late = mark & 15 & ~out
                one = one + lax.population_count(root)
                two = two + lax.population_count(out)
                three = three + lax.population_count(out | late)
                ones, twos = root | late, out & ~root
                for q in range(4):
                    state = ((ones >> q) & 1) | (((twos << 1) >> q) & 2)
                    status[q, pl.ds(b * LANES + at, SUB), tile(c)] = state
            return one, two, three

        carry = lax.fori_loop(0, LANES // SUB, settle, carry, unroll=2)
        for q in range(4):
            copies.append(
                pltpu.make_async_copy(
                    status.at[q, pl.ds(b * LANES, LANES), :],
                    status_out.at[q + odd * (3 - 2 * q), pl.ds(b * LANES, LANES), :],
                    sems.at[4 * b + q],
                )
            )
            copies[-1].start()
    lane = lax.broadcasted_iota(I32, (1, LANES), 1)
    total = jnp.zeros((1, LANES), I32)
    for k in range(3):
        total = jnp.where(lane == k, 4 * height * width - jnp.sum(carry[k]), total)
    count_out[...] = jnp.broadcast_to(total, count_out.shape)
    for c in copies:
        c.wait()


def finish(where, starts, far, near, own, mate, turned, bits, ahead, behind, fan):
    height, width = own.shape[1:]
    tiles, blocks = width // LANES, height // LANES
    args = [in_vmem(x) for x in (*far, *near, own, mate, turned, bits, ahead, behind)]
    return pl.pallas_call(
        functools.partial(finish_kernel, spec=(height, width, starts)),
        compiler_params=GRANT,
        in_specs=[smem(), *vmem(len(args))],
        out_specs=[pl.BlockSpec(memory_space=pl.ANY), vmem(1)[0]],
        out_shape=[
            jax.ShapeDtypeStruct((4, height, width), I32),
            VMEM((fan, LANES), I32),
        ],
        scratch_shapes=[
            VMEM((blocks, width + 2 * SUB, LANES), I32),
            VMEM((tiles, height + 2 * SUB, LANES), I32),
            VMEM((tiles, height, LANES), I32),
            VMEM((4 * tiles, height + 2 * SUB, LANES), U32),
            VMEM((4, width + 2 * SUB, LANES), U32),
            VMEM((width, LANES), I32),
            VMEM((tiles, LANES, LANES), I32),
            VMEM((4, height, width), I32),
            pltpu.SemaphoreType.DMA((4 * blocks,)),
        ],
    )(where, *args)


def pairs(count, swap):
    return [(i, swap(i)) for i in range(count) if 0 <= swap(i) < count]


def shards(scores):
    count = lax.axis_size(GZ)
    height = scores.shape[1]
    blocks = height // LANES
    me = lax.axis_index(GZ)
    odd = me % 2
    edge = (me == 0) | (me == count - 1)
    where = jnp.stack([odd, jnp.where(edge, 0, -1)]).astype(I32)
    over = lambda x: lax.ppermute(x, GZ, pairs(count, lambda i: i - 1 + 2 * (i % 2)))
    swap = lambda x: lax.ppermute(x, GZ, pairs(count, lambda i: i ^ 1))

    early = EARLY if 0 < EARLY < blocks else 0
    starts = (0, early * LANES + SUB)
    ends = (*starts[1:], height)
    firsts, lasts = (0, early), (early, blocks)

    scores = pltpu.with_memory_space_constraint(scores, pltpu.HBM)
    near, words = cut(where, scores, (("near", 0, ends[0]),))
    far = [unpack(over(words[0]), ends[0])]
    rest = [("near", a, b) for a, b in zip(starts[1:], ends[1:])]
    (*more, own), words = cut(
        where, scores, (*rest, ("own", 0, height)), (in_vmem(near[0]),)
    )
    near = [*near, *more]
    late = over(words[0])
    mate = swap(own)
    turned = turn(starts, near, own)

    found = ()
    for a, b in zip(firsts, lasts):
        if a:
            far.append(unpack(late, height - starts[1], (found[0],)))
        found = find_roots(where, a, b, starts, far, near, own, mate, turned, found)
    bits, ahead, behind = found
    status, part = finish(
        where, starts, far, near, own, mate, turned, bits, over(ahead), swap(behind), count
    )
    total = jnp.sum(lax.all_to_all(part, GZ, 0, 0, tiled=True), axis=0)
    return status, total[:3]


def solution(mesh):
    finer = Mesh(mesh.devices.reshape(4, 4, 4, 2), GZ)
    return jax.shard_map(
        shards, mesh=finer, in_specs=(P(GZ, None, None),), out_specs=(P(GZ, None, None), P()),
        check_vma=False,
    )
```
